32 devices in a mesh: img: 4 (over x, core), slab: 8 (over z, y).
Axes of the slice: x: 2, y: 2, z: 4, core: 2. Of those that a mesh axis runs over, the one named last changes fastest.
Arguments:
- section_input: bfloat16 [256, 256, 1024], P(('img', 'slab')), parts along dimension 0, may hold values from -54 to 54
- w_reduce: bfloat16 [3, 1024, 256], replicated, may hold values from -0.1875 to 0.1875
- w_spatial: bfloat16 [3, 9, 256, 256], replicated, may hold values from -0.125 to 0.125
- w_expand: bfloat16 [3, 256, 1024], replicated, may hold values from -0.375 to 0.375
- gain_mid: float32 [3, 2, 256], replicated, may hold values from 0.25 to 1.75
- shift_mid: float32 [3, 2, 256], replicated, may hold values from -3 to 3
- gain_out: float32 [3, 1024], replicated, may hold values from 0.25 to 1.75
- shift_out: float32 [3, 1024], replicated, may hold values from -3 to 3
Outputs:
- section_output: bfloat16 [256, 256, 1024], P(('img', 'slab')), parts along dimension 0
The draws below stay inside these ranges and needn't reach their ends.
There are 4 independent parts, one for each index of `img`. The reference program is written for one: setup_inputs(seed, part) draws one part's arguments, and reference() takes and returns one part's arrays. A program takes and returns all parts, laid end to end along the dimension named above; an argument that names none is the same for every part. Nothing has to cross between parts.
All inputs are finite; a program needn't handle non-finite values.
Results may differ from the reference program's by a relative error of at most 0.01.
Values may be sent and summed in bfloat16 or wider, within the bound.
A program may use at most 128 MiB of HBM per device.

```python
import jax
import jax.numpy as jnp
from jax import lax

C = 1024
CM = 256
W = 256
LAYERS = 3
H = 64


def draw_section_input(key, part):
    positions = jnp.arange(H, dtype=jnp.float32) / max(H - 1, 1)
    noise = jnp.clip(jax.random.normal(key, (H, W, C), jnp.float32), -6.0, 6.0)
    scale = jnp.exp(positions * jnp.log(3.0))
    return (noise * scale[:, None, None]).astype(jnp.bfloat16)


def scatter_about(rng, shape, scale, most, held_as=jnp.bfloat16):
    return jnp.clip(scale * jax.random.normal(rng, shape, jnp.float32), -most, most).astype(held_as)


def setup_inputs(seed: int = 0, part: int = 0) -> dict:
    arg_keys = jax.random.split(jax.random.key(seed), 9)
    part_splits = jax.random.split(jax.random.fold_in(arg_keys[8], part), 9)
    return {
        "section_input": draw_section_input(jax.random.fold_in(jax.random.fold_in(arg_keys[8], part), 71), part),
        "w_reduce": scatter_about(arg_keys[1], (LAYERS, C, CM), C ** -0.5, 0.1875),
        "w_spatial": scatter_about(arg_keys[2], (LAYERS, 9, CM, CM), (9 * CM) ** -0.5, 0.125),
        "w_expand": scatter_about(arg_keys[3], (LAYERS, CM, C), CM ** -0.5, 0.375),
        "gain_mid": jnp.clip(1.0 + 0.15 * jax.random.normal(arg_keys[4], (LAYERS, 2, CM), jnp.float32), 0.25, 1.75),
        "shift_mid": scatter_about(arg_keys[5], (LAYERS, 2, CM), 0.5, 3.0, jnp.float32),
        "gain_out": jnp.clip(1.0 + 0.15 * jax.random.normal(arg_keys[6], (LAYERS, C), jnp.float32), 0.25, 1.75),
        "shift_out": scatter_about(arg_keys[7], (LAYERS, C), 0.5, 3.0, jnp.float32),
    }


def normalize(values, gain, shift):
    mean = lax.optimization_barrier(jnp.mean(values, axis=0))
    var = lax.optimization_barrier(jnp.mean(jnp.square(values - mean), axis=0))
    return (values - mean) * jax.lax.rsqrt(var + 1e-05) * gain + shift

def spatial_conv(hidden, taps):
    rows, width, mid = hidden.shape
    padded = jnp.pad(hidden, ((1, 1), (1, 1), (0, 0)))
    total = jnp.zeros((rows * width, taps.shape[2]), jnp.float32)
    for down in range(3):
        for across in range(3):
            window = padded[down:down + rows, across:across + width].reshape(-1, mid)
            total = total + jnp.dot(window, taps[3 * down + across], preferred_element_type=jnp.float32)
    return total

def reference(section_input, w_reduce, w_spatial, w_expand, gain_mid, shift_mid, gain_out, shift_out):
    rows, width, chans = section_input.shape
    mid = w_reduce.shape[2]
    current = section_input
    for layer in range(LAYERS):
        flat = current.reshape(-1, chans)
        reduced = jnp.dot(flat, w_reduce[layer], preferred_element_type=jnp.float32)
        hidden = jnp.maximum(normalize(reduced, gain_mid[layer, 0], shift_mid[layer, 0]), 0.0).astype(jnp.bfloat16)
        spatial = spatial_conv(hidden.reshape(rows, width, mid), w_spatial[layer])
        inner = jnp.maximum(normalize(spatial, gain_mid[layer, 1], shift_mid[layer, 1]), 0.0).astype(jnp.bfloat16)
        expanded = jnp.dot(inner, w_expand[layer], preferred_element_type=jnp.float32)
        summed = normalize(expanded, gain_out[layer], shift_out[layer]) + flat.astype(jnp.float32)
        current = jnp.maximum(summed, 0.0).astype(jnp.bfloat16).reshape(rows, width, chans)
    return current
```

```python
import functools

import jax
import jax.numpy as jnp
from jax import lax
from jax.experimental import pallas as pl
from jax.experimental.pallas import tpu as pltpu
from jax.sharding import PartitionSpec as P

MESH = pl.DeviceIdType.MESH
EPS = 1e-05
REDUCE_ROWS = 2
CONV_ROWS = 2
EXPAND_ROWS = 1
OUTPUT_ROWS = 1
FINAL_ROWS = 1
LANES = 8
GROUP = 2


def divisor(rows, most):
    return max(d for d in range(1, most + 1) if rows % d == 0)


def kernel(
    n, x_hbm, wr_hbm, ws_hbm, we_hbm, gain_mid, shift_mid, gain_out, shift_out,
    expanded, x, last,
    wr, ws, we, red, taps, inner, halo_out, halo_in, stat_out, stat, sums,
    x_sem, w_sem, halo_send, halo_recv, stat_send, stat_recv,
):
    chunks, count, mid = x.shape
    rows, width, chans = x_hbm.shape
    layers = wr.shape[0]
    group = divisor(chunks, GROUP)
    groups = chunks // group
    wide = group * mid
    stages = 2 + groups
    me = lax.axis_index("slab")
    inv_local = 1.0 / count
    inv_count = 1.0 / (count * n)

    def peer(k):
        return lax.rem(me + k, n)

    barrier = pltpu.get_barrier_semaphore()
    for k in range(1, n):
        pl.semaphore_signal(barrier, inc=1, device_id={"slab": peer(k)}, device_id_type=MESH)

    def weight_copy(kind, layer):
        source, target = ((wr_hbm, wr), (ws_hbm, ws), (we_hbm, we))[kind]
        return pltpu.make_async_copy(source.at[layer], target.at[layer], w_sem.at[kind, layer])

    def x_copy(row, c):
        return pltpu.make_async_copy(
            x_hbm.at[row, :, pl.ds(c * mid, mid)],
            x.at[c, pl.ds(row * width, width), :],
            x_sem.at[row, c],
        )

    weight_copy(0, 0).start()
    for row in range(rows):
        for c in range(chunks):
            x_copy(row, c).start()

    def span(row, many=1):
        return pl.ds(row * width, many * width)

    def stat_copy(stage, cols, k):
        return pltpu.make_async_remote_copy(
            src_ref=stat_out.at[stage],
            dst_ref=stat.at[stage, k],
            send_sem=stat_send.at[stage],
            recv_sem=stat_recv.at[stage],
            device_id={"slab": peer(k)},
            device_id_type=MESH,
        )

    def all_stats(stage, sem):
        others = stat.at[stage, pl.ds(1, n - 1)]
        return pltpu.make_async_copy(others, others, sem.at[stage])

    def fold(carry, y):
        y = y.reshape(-1, LANES, 8, y.shape[-1])
        return carry[0] + jnp.sum(y, axis=0), carry[1] + jnp.sum(y * y, axis=0)

    def zeros(cols):
        zero = jnp.zeros((LANES, 8, cols), jnp.float32)
        return zero, zero

    def total(part):
        return jnp.sum(jnp.sum(part, axis=0), axis=0, keepdims=True)

    def send_stats(stage, carry):
        first = total(carry[0])
        both = jnp.concatenate([first, total(carry[1])], axis=0)
        cols = both.shape[-1]
        stat_out[stage, :, 0:cols] = both
        stat[stage, 0, :, 0:cols] = both
        for k in range(1, n):
            stat_copy(stage, cols, k).start()
        return first

    def affine(stage, gain, shift):
        all_stats(stage, stat_recv).wait()
        cols = gain.shape[-1]
        both = jnp.sum(stat[stage], axis=0)[:, 0:cols]
        mean = both[0:1] * inv_count
        var = jnp.maximum(both[1:2] * inv_count - mean * mean, 0.0)
        scale = lax.rsqrt(var + EPS) * gain
        return scale, shift - mean * scale

    def halo_copy(layer, side):
        return pltpu.make_async_remote_copy(
            src_ref=halo_out.at[layer, side],
            dst_ref=halo_in.at[layer, 1 - side],
            send_sem=halo_send.at[layer, side],
            recv_sem=halo_recv.at[layer, 1 - side],
            device_id={"slab": peer(n - 1 if side == 0 else 1)},
            device_id_type=MESH,
        )

    def halo_arrival(layer, side):
        return pltpu.make_async_remote_copy(
            src_ref=halo_out.at[layer, side],
            dst_ref=halo_in.at[layer, side],
            send_sem=halo_send.at[layer, side],
            recv_sem=halo_recv.at[layer, side],
            device_id={"slab": peer(n - 1 if side == 0 else 1)},
            device_id_type=MESH,
        )

    def has_neighbour(side):
        return me > 0 if side == 0 else me < n - 1

    edge = lax.broadcasted_iota(jnp.int32, (16, mid), 0)

    def store_taps(row, h):
        at = span(row)
        before = pltpu.roll(h, 1, 0)
        after = pltpu.roll(h, width - 1, 0)
        taps[at, mid : 2 * mid] = h.astype(jnp.bfloat16)
        before = jnp.concatenate([jnp.where(edge == 0, 0.0, before[0:16]), before[16:]], axis=0)
        taps[at, 0:mid] = before.astype(jnp.bfloat16)
        after = jnp.concatenate(
            [after[: width - 16], jnp.where(edge == 15, 0.0, after[width - 16 :])], axis=0
        )
        taps[at, 2 * mid : 3 * mid] = after.astype(jnp.bfloat16)

    def keep_sums(carry):
        sums[0] = carry[0]
        sums[1] = carry[1]

    for side in range(2):
        row = 0 if side == 0 else rows + 1
        taps[span(row), :] = jnp.zeros((width, 3 * mid), jnp.bfloat16)

    weight_copy(0, 0).wait()
    carry = zeros(mid)
    reduce_rows = divisor(rows, REDUCE_ROWS)
    for row in range(0, rows, reduce_rows):
        for r in range(row, row + reduce_rows):
            for c in range(chunks):
                x_copy(r, c).wait()
        for r in range(row, row + reduce_rows):
            y = jnp.dot(
                jnp.concatenate([x[c, span(r), :] for c in range(chunks)], axis=1),
                wr[0],
                preferred_element_type=jnp.float32,
            )
            red[span(r), :] = y
            carry = fold(carry, y)
    keep_sums(carry)
    pl.semaphore_wait(barrier, n - 1)

    def layer_step(layer, _):
        first = layer * stages

        local_mean = send_stats(first, (sums[0], sums[1])) * inv_local
        for side in range(2):
            row = 0 if side == 0 else rows - 1
            halo_out[layer, side] = (red[span(row), :] - local_mean).astype(jnp.bfloat16)

            @pl.when(has_neighbour(side))
            def _():
                halo_copy(layer, side).start()

        weight_copy(1, layer).start()
        weight_copy(2, layer).start()

        @pl.when(layer < layers - 1)
        def _():
            weight_copy(0, layer + 1).start()

        weight_copy(1, layer).wait()
        scale, shift = affine(first, gain_mid[layer, 0:1], shift_mid[layer, 0:1])

        def hidden(row):
            store_taps(row + 1, jnp.maximum(red[span(row), :] * scale + shift, 0.0))

        def conv(row, many):
            y = jnp.dot(
                jnp.concatenate([taps[span(row + down, many), :] for down in range(3)], axis=1),
                ws[layer].reshape(9 * mid, mid),
                preferred_element_type=jnp.float32,
            )
            red[span(row, many), :] = y
            return y

        carry = zeros(mid)
        done = 0
        conv_rows = divisor(rows - 2, CONV_ROWS)
        for row in range(1, rows - 1, conv_rows):
            while done < row + conv_rows + 1:
                hidden(done)
                done += 1
            for r in range(row, row + conv_rows):
                carry = fold(carry, conv(r, 1))

        for side in range(2):
            row = 0 if side == 0 else rows + 1

            @pl.when(has_neighbour(side))
            def _():
                halo_copy(layer, side).wait_send()
                halo_arrival(layer, side).wait_recv()
                theirs = stat[first, 1 if side == 0 else n - 1, 0:1, 0:mid] * inv_local
                y = halo_in[layer, side].astype(jnp.float32) + theirs
                store_taps(row, jnp.maximum(y * scale + shift, 0.0))

        for row in (0, rows - 1):
            carry = fold(carry, conv(row, 1))
        send_stats(first + 1, carry)

        weight_copy(2, layer).wait()
        scale, shift = affine(first + 1, gain_mid[layer, 1:2], shift_mid[layer, 1:2])

        expand_rows = divisor(rows, EXPAND_ROWS)
        for g in range(groups):
            parts = [zeros(mid) for _ in range(group)]
            for row in range(0, rows, expand_rows):
                at = span(row, expand_rows)
                if g == 0:
                    block = jnp.maximum(red[at, :] * scale + shift, 0.0).astype(jnp.bfloat16)
                    inner[at, :] = block
                else:
                    block = inner[at, :]
                for i in range(group):
                    c = g * group + i
                    y = jnp.dot(
                        block, we[layer, :, c * mid : (c + 1) * mid],
                        preferred_element_type=jnp.float32,
                    )
                    expanded[c, at, :] = y
                    parts[i] = fold(parts[i], y)
            send_stats(
                first + 2 + g,
                tuple(jnp.concatenate([p[j] for p in parts], axis=-1) for j in range(2)),
            )

        @pl.when(layer < layers - 1)
        def _():
            weight_copy(0, layer + 1).wait()

        output_rows = divisor(rows, OUTPUT_ROWS)
        carry = zeros(mid)
        for g in range(groups):
            cols = slice(g * wide, (g + 1) * wide)
            scale, shift = affine(
                first + 2 + g, gain_out[pl.ds(layer, 1), cols], shift_out[pl.ds(layer, 1), cols]
            )

            @pl.when(layer == layers - 1)
            def _():
                last[0:1, cols] = scale
                last[1:2, cols] = shift

            @pl.when(layer < layers - 1)
            def _():
                carry = zeros(mid)
                for row in range(0, rows, output_rows):
                    at = span(row, output_rows)
                    blocks = []
                    for i in range(group):
                        c = g * group + i
                        part = slice(i * mid, (i + 1) * mid)
                        y = expanded[c, at, :] * scale[:, part] + shift[:, part]
                        y = y + x[c, at, :].astype(jnp.float32)
                        y = jnp.maximum(y, 0.0).astype(jnp.bfloat16)
                        x[c, at, :] = y
                        blocks.append(y)
                    y = jnp.dot(
                        jnp.concatenate(blocks, axis=1),
                        wr[layer + 1, cols, :],
                        preferred_element_type=jnp.float32,
                    )
                    if g > 0:
                        y = y + red[at, :]
                    red[at, :] = y
                    if g == groups - 1:
                        carry = fold(carry, y)
                if g == groups - 1:
                    keep_sums(carry)

        for stage in range(stages):
            all_stats(first + stage, stat_send).wait()
        return 0

    lax.fori_loop(0, layers, layer_step, 0)


def finish(expanded, x, last, out_hbm, buffer, out_sem):
    chunks, count, mid = x.shape
    rows, width, chans = out_hbm.shape
    many = divisor(rows, FINAL_ROWS)

    def out_copy(row):
        at = pl.ds(row, many)
        return pltpu.make_async_copy(buffer.at[at], out_hbm.at[at], out_sem.at[row // many])

    for row in range(0, rows, many):
        at = pl.ds(row * width, many * width)
        for c in range(chunks):
            cols = slice(c * mid, (c + 1) * mid)
            y = expanded[c, at, :] * last[0:1, cols] + last[1:2, cols]
            y = jnp.maximum(y + x[c, at, :].astype(jnp.float32), 0.0)
            buffer[pl.ds(row, many), :, cols] = y.astype(jnp.bfloat16).reshape(many, width, mid)
        out_copy(row).start()
    for row in range(0, rows, many):
        out_copy(row).wait()


def solution(mesh):
    n = mesh.shape["slab"]

    def local(section_input, w_reduce, w_spatial, w_expand, gain_mid, shift_mid, gain_out, shift_out):
        rows, width, chans = section_input.shape
        layers, _, mid = w_reduce.shape
        chunks = chans // mid
        group = divisor(chunks, GROUP)
        count = rows * width
        stages = layers * (2 + chunks // group)
        wide = group * mid
        bf16, f32 = jnp.bfloat16, jnp.float32
        hbm = pl.BlockSpec(memory_space=pl.ANY)
        vmem = pl.BlockSpec(memory_space=pltpu.VMEM)
        held = pl.pallas_call(
            functools.partial(kernel, n),
            out_shape=[
                pltpu.VMEM((chunks, count, mid), f32),
                pltpu.VMEM((chunks, count, mid), bf16),
                pltpu.VMEM((2, chans), f32),
            ],
            in_specs=[hbm] * 4 + [vmem] * 4,
            out_specs=[vmem] * 3,
            scratch_shapes=[
                pltpu.VMEM(w_reduce.shape, bf16),
                pltpu.VMEM(w_spatial.shape, bf16),
                pltpu.VMEM(w_expand.shape, bf16),
                pltpu.VMEM((count, mid), f32),
                pltpu.VMEM(((rows + 2) * width, 3 * mid), bf16),
                pltpu.VMEM((count, mid), bf16),
                pltpu.VMEM((layers, 2, width, mid), bf16),
                pltpu.VMEM((layers, 2, width, mid), bf16),
                pltpu.VMEM((stages, 2, wide), f32),
                pltpu.VMEM((stages, n, 2, wide), f32),
                pltpu.VMEM((2, LANES, 8, mid), f32),
                pltpu.SemaphoreType.DMA((rows, chunks)),
                pltpu.SemaphoreType.DMA((3, layers)),
                pltpu.SemaphoreType.DMA((layers, 2)),
                pltpu.SemaphoreType.DMA((layers, 2)),
                pltpu.SemaphoreType.DMA((stages,)),
                pltpu.SemaphoreType.DMA((stages,)),
            ],
            compiler_params=pltpu.CompilerParams(
                collective_id=0, has_side_effects=True, vmem_limit_bytes=40 * 1024 * 1024
            ),
            name="blocks",
        )(section_input, w_reduce, w_spatial, w_expand, gain_mid, shift_mid, gain_out, shift_out)
        held = [pltpu.with_memory_space_constraint(a, pltpu.VMEM) for a in held]
        return pl.pallas_call(
            finish,
            out_shape=jax.ShapeDtypeStruct(section_input.shape, bf16),
            in_specs=[vmem] * 3,
            out_specs=hbm,
            scratch_shapes=[
                pltpu.VMEM((rows, width, chans), bf16),
                pltpu.SemaphoreType.DMA((rows // divisor(rows, FINAL_ROWS),)),
            ],
            compiler_params=pltpu.CompilerParams(vmem_limit_bytes=16 * 1024 * 1024),
            name="finish",
        )(*held)

    placed = (P(("img", "slab"), None, None), P(), P(), P(), P(), P(), P(), P())
    return jax.shard_map(
        local, mesh=mesh, in_specs=placed, out_specs=P(("img", "slab"), None, None), check_vma=False
    )
```

```python
import functools

import jax
import jax.numpy as jnp
from jax import lax
from jax.experimental import pallas as pl
from jax.experimental.pallas import tpu as pltpu
from jax.sharding import PartitionSpec as P

MESH = pl.DeviceIdType.MESH
EPS = 1e-05
REDUCE_ROWS = 2
CONV_ROWS = 2
EXPAND_ROWS = 1
OUTPUT_ROWS = 1
LANES = 2
GROUP = 2


def divisor(rows, most):
    return max(d for d in range(1, most + 1) if rows % d == 0)


def kernel(
    n, x_hbm, wr_hbm, ws_hbm, we_hbm, gain_mid_hbm, shift_mid_hbm, gain_out_hbm, shift_out_hbm,
    expanded, x, last,
    gain_mid, shift_mid, gain_out, shift_out, wr, ws, we, red, taps, inner, halo_out, halo_in, stat_out, stat, sums,
    g_sem, x_sem, w_sem, halo_send, halo_recv, stat_send, stat_recv,
):
    chunks, rows, width, mid = x.shape
    count = rows * width
    layers = wr.shape[0]
    group = divisor(chunks, GROUP)
    groups = chunks // group
    wide = group * mid
    stages = 2 + groups
    me = lax.axis_index("slab")
    inv_local = 1.0 / count
    inv_count = 1.0 / (count * n)

    def peer(k):
        return lax.rem(me + k, n)

    barrier = pltpu.get_barrier_semaphore()
    for k in range(1, n):
        pl.semaphore_signal(barrier, inc=1, device_id={"slab": peer(k)}, device_id_type=MESH)

    def weight_copy(kind, layer):
        source, target = ((wr_hbm, wr), (ws_hbm, ws), (we_hbm, we))[kind]
        return pltpu.make_async_copy(source.at[layer], target.at[layer], w_sem.at[kind])

    reduce_rows = divisor(rows, REDUCE_ROWS)

    def x_copy(step, c):
        at = pl.ds(step * reduce_rows, reduce_rows)
        return pltpu.make_async_copy(
            x_hbm.at[at, :, pl.ds(c * mid, mid)], x.at[c, at], x_sem.at[step]
        )

    def x_arrival(step):
        whole = x.at[:, pl.ds(step * reduce_rows, reduce_rows)]
        return pltpu.make_async_copy(whole, whole, x_sem.at[step])

    small = [
        pltpu.make_async_copy(source, target, g_sem.at[i])
        for i, (source, target) in enumerate(
            (
                (gain_mid_hbm, gain_mid),
                (shift_mid_hbm, shift_mid),
                (gain_out_hbm, gain_out),
                (shift_out_hbm, shift_out),
            )
        )
    ]
    weight_copy(0, 0).start()
    for step in range(rows // reduce_rows):
        for c in range(chunks):
            x_copy(step, c).start()
    for copy in small:
        copy.start()

    def span(row, many=1):
        return pl.ds(row * width, many * width)

    def stat_copy(stage, kind, k):
        return pltpu.make_async_remote_copy(
            src_ref=stat_out.at[stage],
            dst_ref=stat.at[stage, k],
            send_sem=stat_send.at[kind],
            recv_sem=stat_recv.at[kind],
            device_id={"slab": peer(k)},
            device_id_type=MESH,
        )

    def all_stats(stage, kind, sem):
        others = stat.at[stage, pl.ds(1, n - 1)]
        return pltpu.make_async_copy(others, others, sem.at[kind])

    def fold(carry, y):
        y = y.reshape(-1, LANES, 8, y.shape[-1])
        return carry[0] + jnp.sum(y, axis=0), carry[1] + jnp.sum(y * y, axis=0)

    def zeros(cols):
        zero = jnp.zeros((LANES, 8, cols), jnp.float32)
        return zero, zero

    order = sorted(range(1, n), key=lambda k: (1 - k % 2, -abs(2 * k - n)))

    def total(part):
        return jnp.sum(jnp.sum(part, axis=0), axis=0, keepdims=True)

    def send_stats(layer, kind, carry):
        stage = layer * stages + kind
        first = total(carry[0])
        both = jnp.concatenate([first, total(carry[1])], axis=0)
        cols = both.shape[-1]
        stat_out[stage, :, 0:cols] = both
        stat[stage, 0, :, 0:cols] = both
        for k in order:
            stat_copy(stage, kind, k).start()
        return first

    def affine(layer, kind, gain, shift):
        stage = layer * stages + kind
        all_stats(stage, kind, stat_recv).wait()
        cols = gain.shape[-1]
        both = jnp.sum(stat[stage], axis=0)[:, 0:cols]
        mean = both[0:1] * inv_count
        var = jnp.maximum(both[1:2] * inv_count - mean * mean, 0.0)
        scale = lax.rsqrt(var + EPS) * gain
        return scale, shift - mean * scale

    def halo_copy(layer, side):
        return pltpu.make_async_remote_copy(
            src_ref=halo_out.at[layer, side],
            dst_ref=halo_in.at[layer, 1 - side],
            send_sem=halo_send.at[side],
            recv_sem=halo_recv.at[1 - side],
            device_id={"slab": peer(n - 1 if side == 0 else 1)},
            device_id_type=MESH,
        )

    def halo_arrival(layer, side):
        return pltpu.make_async_remote_copy(
            src_ref=halo_out.at[layer, side],
            dst_ref=halo_in.at[layer, side],
            send_sem=halo_send.at[side],
            recv_sem=halo_recv.at[side],
            device_id={"slab": peer(n - 1 if side == 0 else 1)},
            device_id_type=MESH,
        )

    def has_neighbour(side):
        return me > 0 if side == 0 else me < n - 1

    edge = lax.broadcasted_iota(jnp.int32, (16, mid), 0)

    def store_taps(row, h):
        at = span(row)
        before = pltpu.roll(h, 1, 0)
        after = pltpu.roll(h, width - 1, 0)
        taps[at, mid : 2 * mid] = h.astype(jnp.bfloat16)
        before = jnp.concatenate([jnp.where(edge == 0, 0.0, before[0:16]), before[16:]], axis=0)
        taps[at, 0:mid] = before.astype(jnp.bfloat16)
        after = jnp.concatenate(
            [after[: width - 16], jnp.where(edge == 15, 0.0, after[width - 16 :])], axis=0
        )
        taps[at, 2 * mid : 3 * mid] = after.astype(jnp.bfloat16)

    def keep_sums(carry):
        sums[0] = carry[0]
        sums[1] = carry[1]

    for side in range(2):
        row = 0 if side == 0 else rows + 1
        taps[span(row), :] = jnp.zeros((width, 3 * mid), jnp.bfloat16)

    weight_copy(0, 0).wait()
    carry = zeros(mid)
    for row in range(0, rows, reduce_rows):
        x_arrival(row // reduce_rows).wait()
        for r in range(row, row + reduce_rows):
            y = jnp.dot(
                jnp.concatenate([x[c, r] for c in range(chunks)], axis=1),
                wr[0],
                preferred_element_type=jnp.float32,
            )
            red[span(r), :] = y
            carry = fold(carry, y)
    keep_sums(carry)
    for copy in small:
        copy.wait()
    pl.semaphore_wait(barrier, n - 1)

    def layer_step(layer, _):
        first = layer * stages

        local_mean = send_stats(layer, 0, (sums[0], sums[1])) * inv_local
        for side in range(2):
            row = 0 if side == 0 else rows - 1
            halo_out[layer, side] = (red[span(row), :] - local_mean).astype(jnp.bfloat16)

            @pl.when(has_neighbour(side))
            def _():
                halo_copy(layer, side).start()

        weight_copy(1, layer).start()
        weight_copy(2, layer).start()

        @pl.when(layer < layers - 1)
        def _():
            weight_copy(0, layer + 1).start()

        weight_copy(1, layer).wait()
        scale, shift = affine(layer, 0, gain_mid[layer, 0:1], shift_mid[layer, 0:1])

        def hidden(row):
            store_taps(row + 1, jnp.maximum(red[span(row), :] * scale + shift, 0.0))

        def conv(row, many):
            y = jnp.dot(
                jnp.concatenate([taps[span(row + down, many), :] for down in range(3)], axis=1),
                ws[layer].reshape(9 * mid, mid),
                preferred_element_type=jnp.float32,
            )
            red[span(row, many), :] = y
            return y

        carry = zeros(mid)
        done = 0
        conv_rows = divisor(rows - 2, CONV_ROWS)
        for row in range(1, rows - 1, conv_rows):
            while done < row + conv_rows + 1:
                hidden(done)
                done += 1
            for r in range(row, row + conv_rows):
                carry = fold(carry, conv(r, 1))

        for side in range(2):
            row = 0 if side == 0 else rows + 1

            @pl.when(has_neighbour(side))
            def _():
                halo_copy(layer, side).wait_send()
                halo_arrival(layer, side).wait_recv()
                theirs = stat[first, 1 if side == 0 else n - 1, 0:1, 0:mid] * inv_local
                y = halo_in[layer, side].astype(jnp.float32) + theirs
                store_taps(row, jnp.maximum(y * scale + shift, 0.0))

        for row in (0, rows - 1):
            carry = fold(carry, conv(row, 1))
        send_stats(layer, 1, carry)

        weight_copy(2, layer).wait()
        scale, shift = affine(layer, 1, gain_mid[layer, 1:2], shift_mid[layer, 1:2])

        expand_rows = divisor(rows, EXPAND_ROWS)
        for g in range(groups):
            parts = [zeros(mid) for _ in range(group)]
            for row in range(0, rows, expand_rows):
                at = span(row, expand_rows)
                if g == 0:
                    block = jnp.maximum(red[at, :] * scale + shift, 0.0).astype(jnp.bfloat16)
                    inner[at, :] = block
                else:
                    block = inner[at, :]
                for i in range(group):
                    c = g * group + i
                    y = jnp.dot(
                        block, we[layer, :, c * mid : (c + 1) * mid],
                        preferred_element_type=jnp.float32,
                    )
                    expanded[c, at, :] = y
                    parts[i] = fold(parts[i], y)
            send_stats(
                layer,
                2 + g,
                tuple(jnp.concatenate([p[j] for p in parts], axis=-1) for j in range(2)),
            )

        @pl.when(layer < layers - 1)
        def _():
            weight_copy(0, layer + 1).wait()

        output_rows = divisor(rows, OUTPUT_ROWS)
        carry = zeros(mid)
        for g in range(groups):
            cols = slice(g * wide, (g + 1) * wide)
            scale, shift = affine(
                layer, 2 + g, gain_out[pl.ds(layer, 1), cols], shift_out[pl.ds(layer, 1), cols]
            )

            @pl.when(layer == layers - 1)
            def _():
                last[0:1, cols] = scale
                last[1:2, cols] = shift

            @pl.when(layer < layers - 1)
            def _():
                carry = zeros(mid)
                for row in range(0, rows, output_rows):
                    at = span(row, output_rows)
                    blocks = []
                    for i in range(group):
                        c = g * group + i
                        part = slice(i * mid, (i + 1) * mid)
                        y = expanded[c, at, :] * scale[:, part] + shift[:, part]
                        y = jnp.maximum(y.astype(jnp.bfloat16) + x[c, row], 0.0)
                        x[c, row] = y
                        blocks.append(y)
                    y = jnp.dot(
                        jnp.concatenate(blocks, axis=1),
                        wr[layer + 1, cols, :],
                        preferred_element_type=jnp.float32,
                    )
                    if g > 0:
                        y = y + red[at, :]
                    red[at, :] = y
                    if g == groups - 1:
                        carry = fold(carry, y)
                if g == groups - 1:
                    keep_sums(carry)

        for stage in range(stages):
            all_stats(first + stage, stage, stat_send).wait()
        return 0

    lax.fori_loop(0, layers, layer_step, 0)


def finish(expanded, x, last, out_hbm, buffer, out_sem):
    chunks, rows, width, mid = x.shape

    def out_copy(row):
        return pltpu.make_async_copy(buffer.at[row], out_hbm.at[row], out_sem.at[row])

    for row in range(rows):
        at = pl.ds(row * width, width)
        for c in range(chunks):
            cols = slice(c * mid, (c + 1) * mid)
            y = expanded[c, at, :] * last[0:1, cols] + last[1:2, cols]
            buffer[row, :, cols] = jnp.maximum(y.astype(jnp.bfloat16) + x[c, row], 0.0)
        out_copy(row).start()
    for row in range(rows):
        out_copy(row).wait()


def solution(mesh):
    n = mesh.shape["slab"]

    def local(section_input, w_reduce, w_spatial, w_expand, gain_mid, shift_mid, gain_out, shift_out):
        rows, width, chans = section_input.shape
        layers, _, mid = w_reduce.shape
        chunks = chans // mid
        group = divisor(chunks, GROUP)
        count = rows * width
        stages = layers * (2 + chunks // group)
        wide = group * mid
        bf16, f32 = jnp.bfloat16, jnp.float32
        hbm = pl.BlockSpec(memory_space=pl.ANY)
        vmem = pl.BlockSpec(memory_space=pltpu.VMEM)
        held = pl.pallas_call(
            functools.partial(kernel, n),
            out_shape=[
                pltpu.VMEM((chunks, count, mid), f32),
                pltpu.VMEM((chunks, rows, width, mid), bf16),
                pltpu.VMEM((2, chans), f32),
            ],
            in_specs=[hbm] * 8,
            out_specs=[vmem] * 3,
            scratch_shapes=[
                pltpu.VMEM(gain_mid.shape, f32),
                pltpu.VMEM(shift_mid.shape, f32),
                pltpu.VMEM(gain_out.shape, f32),
                pltpu.VMEM(shift_out.shape, f32),
                pltpu.VMEM(w_reduce.shape, bf16),
                pltpu.VMEM(w_spatial.shape, bf16),
                pltpu.VMEM(w_expand.shape, bf16),
                pltpu.VMEM((count, mid), f32),
                pltpu.VMEM(((rows + 2) * width, 3 * mid), bf16),
                pltpu.VMEM((count, mid), bf16),
                pltpu.VMEM((layers, 2, width, mid), bf16),
                pltpu.VMEM((layers, 2, width, mid), bf16),
                pltpu.VMEM((stages, 2, wide), f32),
                pltpu.VMEM((stages, n, 2, wide), f32),
                pltpu.VMEM((2, LANES, 8, mid), f32),
                pltpu.SemaphoreType.DMA((4,)),
                pltpu.SemaphoreType.DMA((rows // divisor(rows, REDUCE_ROWS),)),
                pltpu.SemaphoreType.DMA((3,)),
                pltpu.SemaphoreType.DMA((2,)),
                pltpu.SemaphoreType.DMA((2,)),
                pltpu.SemaphoreType.DMA((stages // layers,)),
                pltpu.SemaphoreType.DMA((stages // layers,)),
            ],
            compiler_params=pltpu.CompilerParams(
                collective_id=0, has_side_effects=True, vmem_limit_bytes=40 * 1024 * 1024
            ),
            name="blocks",
        )(
            *(
                pltpu.with_memory_space_constraint(a, pltpu.HBM)
                for a in (
                    section_input, w_reduce, w_spatial, w_expand,
                    gain_mid, shift_mid, gain_out, shift_out,
                )
            )
        )
        held = [pltpu.with_memory_space_constraint(a, pltpu.VMEM) for a in held]
        return pl.pallas_call(
            finish,
            out_shape=jax.ShapeDtypeStruct(section_input.shape, bf16),
            in_specs=[vmem] * 3,
            out_specs=hbm,
            scratch_shapes=[
                pltpu.VMEM((rows, width, chans), bf16),
                pltpu.SemaphoreType.DMA((rows,)),
            ],
            compiler_params=pltpu.CompilerParams(vmem_limit_bytes=16 * 1024 * 1024),
            name="finish",
        )(*held)

    placed = (P(("img", "slab"), None, None), P(), P(), P(), P(), P(), P(), P())
    return jax.shard_map(
        local, mesh=mesh, in_specs=placed, out_specs=P(("img", "slab"), None, None), check_vma=False
    )
```

```python
import functools

import jax
import jax.numpy as jnp
from jax import lax
from jax.experimental import pallas as pl
from jax.experimental.pallas import tpu as pltpu
from jax.sharding import PartitionSpec as P

MESH = pl.DeviceIdType.MESH
EPS = 1e-05
REDUCE_ROWS = 2
CONV_ROWS = 2
EXPAND_ROWS = 1
LANES = 2
GROUP = 2


def divisor(rows, most):
    return max(d for d in range(1, most + 1) if rows % d == 0)


def kernel(
    n, x_hbm, wr_hbm, ws_hbm, we_hbm, gain_mid_hbm, shift_mid_hbm, gain_out_hbm, shift_out_hbm,
    expanded, x, last,
    gain_mid, shift_mid, gain_out, shift_out, wr, ws, we, red, taps, inner, halo_out, halo_in, stat_out, stat, sums,
    g_sem, x_sem, w_sem, halo_send, halo_recv, stat_send, stat_recv,
):
    chunks, rows, width, mid = x.shape
    count = rows * width
    layers = wr.shape[0]
    group = divisor(chunks, GROUP)
    groups = chunks // group
    wide = group * mid
    stages = 2 + groups
    me = lax.axis_index("slab")
    inv_local = 1.0 / count
    inv_count = 1.0 / (count * n)

    def peer(k):
        return lax.rem(me + k, n)

    barrier = pltpu.get_barrier_semaphore()
    for k in range(1, n):
        pl.semaphore_signal(barrier, inc=1, device_id={"slab": peer(k)}, device_id_type=MESH)

    def weight_copy(kind, layer):
        source, target = ((wr_hbm, wr), (ws_hbm, ws))[kind]
        return pltpu.make_async_copy(source.at[layer], target.at[layer], w_sem.at[kind])

    def expand_copy(layer, c):
        return pltpu.make_async_copy(
            we_hbm.at[layer, :, pl.ds(c * mid, mid)], we.at[layer, c], w_sem.at[2]
        )

    def expand_arrival(layer):
        return pltpu.make_async_copy(we.at[layer], we.at[layer], w_sem.at[2])

    reduce_rows = divisor(rows, REDUCE_ROWS)

    def x_copy(step, c, pick):
        return pltpu.make_async_copy(
            x_hbm.at[pick, :, pl.ds(c * mid, mid)], x.at[c, pick], x_sem.at[step]
        )

    def x_arrival(step):
        whole = x.at[:, pl.ds(step * reduce_rows, reduce_rows)]
        return pltpu.make_async_copy(whole, whole, x_sem.at[step])

    steps = [list(range(i, i + reduce_rows)) for i in range(0, rows, reduce_rows)]

    small = [
        pltpu.make_async_copy(source, target, g_sem.at[i])
        for i, (source, target) in enumerate(
            (
                (gain_mid_hbm, gain_mid),
                (shift_mid_hbm, shift_mid),
                (gain_out_hbm, gain_out),
                (shift_out_hbm, shift_out),
            )
        )
    ]
    weight_copy(0, 0).start()
    for step, picks in enumerate(steps):
        for c in range(chunks):
            x_copy(step, c, pl.ds(picks[0], reduce_rows)).start()
    for copy in small:
        copy.start()

    def span(row, many=1):
        return pl.ds(row * width, many * width)

    def stat_copy(stage, kind, k):
        return pltpu.make_async_remote_copy(
            src_ref=stat_out.at[stage],
            dst_ref=stat.at[stage, k],
            send_sem=stat_send.at[kind],
            recv_sem=stat_recv.at[kind],
            device_id={"slab": peer(k)},
            device_id_type=MESH,
        )

    def all_stats(stage, kind, sem):
        others = stat.at[stage, pl.ds(1, n - 1)]
        return pltpu.make_async_copy(others, others, sem.at[kind])

    def fold(carry, y):
        y = y.reshape(-1, LANES, 8, y.shape[-1])
        return carry[0] + jnp.sum(y, axis=0), carry[1] + jnp.sum(y * y, axis=0)

    def zeros(cols):
        zero = jnp.zeros((LANES, 8, cols), jnp.float32)
        return zero, zero

    order = sorted(range(1, n), key=lambda k: (1 - k % 2, -abs(2 * k - n)))

    def total(part):
        return jnp.sum(jnp.sum(part, axis=0), axis=0, keepdims=True)

    def send_stats(layer, kind, carry):
        stage = layer * stages + kind
        first = total(carry[0])
        both = jnp.concatenate([first, total(carry[1])], axis=0)
        cols = both.shape[-1]
        stat_out[stage, :, 0:cols] = both
        stat[stage, 0, :, 0:cols] = both
        for k in order:
            stat_copy(stage, kind, k).start()
        return first

    def affine(layer, kind, gain, shift):
        stage = layer * stages + kind
        all_stats(stage, kind, stat_recv).wait()
        cols = gain.shape[-1]
        both = jnp.sum(stat[stage], axis=0)[:, 0:cols]
        mean = both[0:1] * inv_count
        var = jnp.maximum(both[1:2] * inv_count - mean * mean, 0.0)
        scale = lax.rsqrt(var + EPS) * gain
        return scale, shift - mean * scale

    def halo_copy(layer, side):
        return pltpu.make_async_remote_copy(
            src_ref=halo_out.at[layer, side],
            dst_ref=halo_in.at[layer, 1 - side],
            send_sem=halo_send.at[side],
            recv_sem=halo_recv.at[1 - side],
            device_id={"slab": peer(n - 1 if side == 0 else 1)},
            device_id_type=MESH,
        )

    def halo_arrival(layer, side):
        return pltpu.make_async_remote_copy(
            src_ref=halo_out.at[layer, side],
            dst_ref=halo_in.at[layer, side],
            send_sem=halo_send.at[side],
            recv_sem=halo_recv.at[side],
            device_id={"slab": peer(n - 1 if side == 0 else 1)},
            device_id_type=MESH,
        )

    def has_neighbour(side):
        return me > 0 if side == 0 else me < n - 1

    edge = lax.broadcasted_iota(jnp.int32, (16, mid), 0)

    def store_taps(row, h):
        at = span(row)
        before = pltpu.roll(h, 1, 0)
        after = pltpu.roll(h, width - 1, 0)
        taps[at, mid : 2 * mid] = h.astype(jnp.bfloat16)
        before = jnp.concatenate([jnp.where(edge == 0, 0.0, before[0:16]), before[16:]], axis=0)
        taps[at, 0:mid] = before.astype(jnp.bfloat16)
        after = jnp.concatenate(
            [after[: width - 16], jnp.where(edge == 15, 0.0, after[width - 16 :])], axis=0
        )
        taps[at, 2 * mid : 3 * mid] = after.astype(jnp.bfloat16)

    def keep_sums(carry):
        sums[0] = carry[0]
        sums[1] = carry[1]

    for side in range(2):

        @pl.when(jnp.logical_not(has_neighbour(side)))
        def _():
            for layer in range(layers):
                halo_in[layer, side] = jnp.zeros((width, mid), jnp.bfloat16)

    weight_copy(0, 0).wait()
    carry = zeros(mid)
    for step, picks in enumerate(steps):
        x_arrival(step).wait()
        for r in picks:
            y = jnp.dot(
                jnp.concatenate([x[c, r] for c in range(chunks)], axis=1),
                wr[0],
                preferred_element_type=jnp.float32,
            )
            red[span(r), :] = y
            carry = fold(carry, y)
    keep_sums(carry)
    for copy in small:
        copy.wait()
    pl.semaphore_wait(barrier, n - 1)

    def layer_step(layer, _):
        first = layer * stages

        local_mean = send_stats(layer, 0, (sums[0], sums[1])) * inv_local
        for side in range(2):
            row = 0 if side == 0 else rows - 1
            halo_out[layer, side] = (red[span(row), :] - local_mean).astype(jnp.bfloat16)

            @pl.when(has_neighbour(side))
            def _():
                halo_copy(layer, side).start()

        weight_copy(1, layer).start()
        for c in range(chunks):
            expand_copy(layer, c).start()

        @pl.when(layer < layers - 1)
        def _():
            weight_copy(0, layer + 1).start()

        weight_copy(1, layer).wait()
        scale, shift = affine(layer, 0, gain_mid[layer, 0:1], shift_mid[layer, 0:1])

        def hidden(row):
            store_taps(row + 1, jnp.maximum(red[span(row), :] * scale + shift, 0.0))

        def conv(row, many):
            y = jnp.dot(
                jnp.concatenate([taps[span(row + down, many), :] for down in range(3)], axis=1),
                ws[layer].reshape(9 * mid, mid),
                preferred_element_type=jnp.float32,
            )
            red[span(row, many), :] = y
            return y

        def conv_edge(side, first, many):
            row = 0 if side == 0 else rows - 1
            return jnp.dot(
                jnp.concatenate([taps[span(row + first + i), :] for i in range(many)], axis=1),
                ws[layer, pl.ds(3 * first, 3 * many)].reshape(3 * many * mid, mid),
                preferred_element_type=jnp.float32,
            )

        carry = zeros(mid)
        done = 0
        conv_rows = divisor(rows - 2, CONV_ROWS)
        for row in range(1, rows - 1, conv_rows):
            while done < row + conv_rows + 1:
                hidden(done)
                done += 1
            for r in range(row, row + conv_rows):
                carry = fold(carry, conv(r, 1))
        for side in range(2):
            red[span(0 if side == 0 else rows - 1), :] = conv_edge(side, 1 - side, 2)

        for side in range(2):

            @pl.when(has_neighbour(side))
            def _():
                halo_copy(layer, side).wait_send()
                halo_arrival(layer, side).wait_recv()

        for side in range(2):
            row = 0 if side == 0 else rows + 1
            there = jnp.where(has_neighbour(side), 1.0, 0.0)
            y = halo_in[layer, side].astype(jnp.float32) * (scale * there)
            theirs = stat[first, 1 if side == 0 else n - 1, 0:1, 0:mid] * inv_local
            moved = theirs * scale + shift
            store_taps(row, jnp.maximum(y + moved * there, 0.0))

        for side in range(2):
            at = span(0 if side == 0 else rows - 1)
            y = conv_edge(side, 2 * side, 1) + red[at, :]
            red[at, :] = y
            carry = fold(carry, y)
        send_stats(layer, 1, carry)

        expand_arrival(layer).wait()
        scale, shift = affine(layer, 1, gain_mid[layer, 1:2], shift_mid[layer, 1:2])

        expand_rows = divisor(rows, EXPAND_ROWS)
        for g in range(groups):
            parts = [zeros(mid) for _ in range(group)]
            for row in range(0, rows, expand_rows):
                at = span(row, expand_rows)
                if g == 0:
                    block = jnp.maximum(red[at, :] * scale + shift, 0.0).astype(jnp.bfloat16)
                    inner[at, :] = block
                else:
                    block = inner[at, :]
                for i in range(group):
                    c = g * group + i
                    y = jnp.dot(
                        block, we[layer, c],
                        preferred_element_type=jnp.float32,
                    )
                    expanded[c, at, :] = y
                    parts[i] = fold(parts[i], y)
            send_stats(
                layer,
                2 + g,
                tuple(jnp.concatenate([p[j] for p in parts], axis=-1) for j in range(2)),
            )

        @pl.when(layer < layers - 1)
        def _():
            weight_copy(0, layer + 1).wait()

        carry = zeros(mid)
        for g in range(groups):
            cols = slice(g * wide, (g + 1) * wide)
            scale, shift = affine(
                layer, 2 + g, gain_out[pl.ds(layer, 1), cols], shift_out[pl.ds(layer, 1), cols]
            )

            @pl.when(layer == layers - 1)
            def _():
                last[0:1, cols] = scale
                last[1:2, cols] = shift

            @pl.when(layer < layers - 1)
            def _():
                carry = zeros(mid)
                for row in range(rows):
                    at = span(row)
                    blocks = []
                    for i in range(group):
                        c = g * group + i
                        part = slice(i * mid, (i + 1) * mid)
                        y = expanded[c, at, :] * scale[:, part] + shift[:, part]
                        y = jnp.maximum(y.astype(jnp.bfloat16) + x[c, row], 0.0)
                        x[c, row] = y
                        blocks.append(y)
                    y = jnp.dot(
                        jnp.concatenate(blocks, axis=1),
                        wr[layer + 1, cols, :],
                        preferred_element_type=jnp.float32,
                    )
                    if g > 0:
                        y = y + red[at, :]
                    red[at, :] = y
                    if g == groups - 1:
                        carry = fold(carry, y)
                if g == groups - 1:
                    keep_sums(carry)

        for stage in range(stages):
            all_stats(first + stage, stage, stat_send).wait()
        return 0

    lax.fori_loop(0, layers, layer_step, 0)


def finish(expanded, x, last, out_hbm, buffer, out_sem):
    chunks, rows, width, mid = x.shape

    def out_copy(row):
        return pltpu.make_async_copy(buffer.at[row], out_hbm.at[row], out_sem.at[row])

    for row in range(rows):
        at = pl.ds(row * width, width)
        for c in range(chunks):
            cols = slice(c * mid, (c + 1) * mid)
            y = expanded[c, at, :] * last[0:1, cols] + last[1:2, cols]
            buffer[row, :, cols] = jnp.maximum(y.astype(jnp.bfloat16) + x[c, row], 0.0)
        out_copy(row).start()
    for row in range(rows):
        out_copy(row).wait()


def solution(mesh):
    n = mesh.shape["slab"]

    def local(section_input, w_reduce, w_spatial, w_expand, gain_mid, shift_mid, gain_out, shift_out):
        rows, width, chans = section_input.shape
        layers, _, mid = w_reduce.shape
        chunks = chans // mid
        group = divisor(chunks, GROUP)
        count = rows * width
        stages = layers * (2 + chunks // group)
        wide = group * mid
        bf16, f32 = jnp.bfloat16, jnp.float32
        hbm = pl.BlockSpec(memory_space=pl.ANY)
        vmem = pl.BlockSpec(memory_space=pltpu.VMEM)
        held = pl.pallas_call(
            functools.partial(kernel, n),
            out_shape=[
                pltpu.VMEM((chunks, count, mid), f32),
                pltpu.VMEM((chunks, rows, width, mid), bf16),
                pltpu.VMEM((2, chans), f32),
            ],
            in_specs=[hbm] * 8,
            out_specs=[vmem] * 3,
            scratch_shapes=[
                pltpu.VMEM(gain_mid.shape, f32),
                pltpu.VMEM(shift_mid.shape, f32),
                pltpu.VMEM(gain_out.shape, f32),
                pltpu.VMEM(shift_out.shape, f32),
                pltpu.VMEM(w_reduce.shape, bf16),
                pltpu.VMEM(w_spatial.shape, bf16),
                pltpu.VMEM((layers, chunks, mid, mid), bf16),
                pltpu.VMEM((count, mid), f32),
                pltpu.VMEM(((rows + 2) * width, 3 * mid), bf16),
                pltpu.VMEM((count, mid), bf16),
                pltpu.VMEM((layers, 2, width, mid), bf16),
                pltpu.VMEM((layers, 2, width, mid), bf16),
                pltpu.VMEM((stages, 2, wide), f32),
                pltpu.VMEM((stages, n, 2, wide), f32),
                pltpu.VMEM((2, LANES, 8, mid), f32),
                pltpu.SemaphoreType.DMA((4,)),
                pltpu.SemaphoreType.DMA((rows // divisor(rows, REDUCE_ROWS),)),
                pltpu.SemaphoreType.DMA((3,)),
                pltpu.SemaphoreType.DMA((2,)),
                pltpu.SemaphoreType.DMA((2,)),
                pltpu.SemaphoreType.DMA((stages // layers,)),
                pltpu.SemaphoreType.DMA((stages // layers,)),
            ],
            compiler_params=pltpu.CompilerParams(
                collective_id=0, has_side_effects=True, vmem_limit_bytes=40 * 1024 * 1024
            ),
            name="blocks",
        )(
            *(
                pltpu.with_memory_space_constraint(a, pltpu.HBM)
                for a in (
                    section_input, w_reduce, w_spatial, w_expand,
                    gain_mid, shift_mid, gain_out, shift_out,
                )
            )
        )
        held = [pltpu.with_memory_space_constraint(a, pltpu.VMEM) for a in held]
        return pl.pallas_call(
            finish,
            out_shape=jax.ShapeDtypeStruct(section_input.shape, bf16),
            in_specs=[vmem] * 3,
            out_specs=hbm,
            scratch_shapes=[
                pltpu.VMEM((rows, width, chans), bf16),
                pltpu.SemaphoreType.DMA((rows,)),
            ],
            compiler_params=pltpu.CompilerParams(vmem_limit_bytes=16 * 1024 * 1024),
            name="finish",
        )(*held)

    placed = (P(("img", "slab"), None, None), P(), P(), P(), P(), P(), P(), P())
    return jax.shard_map(
        local, mesh=mesh, in_specs=placed, out_specs=P(("img", "slab"), None, None), check_vma=False
    )
```

```python
import functools

import jax
import jax.numpy as jnp
from jax import lax
from jax.experimental import pallas as pl
from jax.experimental.pallas import tpu as pltpu
from jax.sharding import PartitionSpec as P

MESH = pl.DeviceIdType.MESH
EPS = 1e-05
REDUCE_ROWS = 2
CONV_ROWS = 2
EXPAND_ROWS = 1
LANES = 2
GROUP = 1


def divisor(rows, most):
    return max(d for d in range(1, most + 1) if rows % d == 0)


def kernel(
    n, x_hbm, wr_hbm, ws_hbm, we_hbm, gain_mid_hbm, shift_mid_hbm, gain_out_hbm, shift_out_hbm,
    expanded, x, last,
    gain_mid, shift_mid, gain_out, shift_out, wr, ws, we, red, taps, inner, halo_out, halo_in, stat_out, stat, sums,
    g_sem, x_sem, w_sem, halo_send, halo_recv, stat_send, stat_recv,
):
    chunks, rows, width, mid = x.shape
    count = rows * width
    layers = wr.shape[0]
    group = divisor(chunks, GROUP)
    groups = chunks // group
    wide = group * mid
    stages = 2 + groups
    me = lax.axis_index("slab")
    inv_local = 1.0 / count
    inv_count = 1.0 / (count * n)

    def peer(k):
        return lax.rem(me + k, n)

    def weight_copy(kind, layer):
        source, target = ((wr_hbm, wr), (ws_hbm, ws))[kind]
        return pltpu.make_async_copy(source.at[layer], target.at[layer], w_sem.at[kind])

    def expand_copy(layer, c):
        return pltpu.make_async_copy(
            we_hbm.at[layer, :, pl.ds(c * mid, mid)], we.at[layer, c], w_sem.at[2]
        )

    def expand_arrival(layer):
        return pltpu.make_async_copy(we.at[layer], we.at[layer], w_sem.at[2])

    reduce_rows = divisor(rows, REDUCE_ROWS)

    def x_copy(step, c, pick):
        return pltpu.make_async_copy(
            x_hbm.at[pick, :, pl.ds(c * mid, mid)], x.at[c, pick], x_sem.at[step]
        )

    def x_arrival(step):
        whole = x.at[:, pl.ds(steps[step][0], len(steps[step]))]
        return pltpu.make_async_copy(whole, whole, x_sem.at[step])

    steps = [list(range(i, i + reduce_rows)) for i in range(0, rows, reduce_rows)]
    if len(steps) > 1:
        steps = steps[:-2] + [steps[-2] + steps[-1]]

    small = [
        pltpu.make_async_copy(source, target, g_sem.at[i])
        for i, (source, target) in enumerate(
            (
                (gain_mid_hbm, gain_mid),
                (shift_mid_hbm, shift_mid),
                (gain_out_hbm, gain_out),
                (shift_out_hbm, shift_out),
            )
        )
    ]
    weight_copy(0, 0).start()
    for step, picks in enumerate(steps):
        for c in range(chunks):
            x_copy(step, c, pl.ds(picks[0], len(picks))).start()
    for copy in small:
        copy.start()

    barrier = pltpu.get_barrier_semaphore()
    for k in range(1, n):
        pl.semaphore_signal(barrier, inc=1, device_id={"slab": peer(k)}, device_id_type=MESH)

    def span(row, many=1):
        return pl.ds(row * width, many * width)

    def stat_copy(stage, kind, k):
        return pltpu.make_async_remote_copy(
            src_ref=stat_out.at[stage],
            dst_ref=stat.at[stage, k],
            send_sem=stat_send.at[kind],
            recv_sem=stat_recv.at[kind],
            device_id={"slab": peer(k)},
            device_id_type=MESH,
        )

    def all_stats(stage, kind, sem):
        others = stat.at[stage, pl.ds(1, n - 1)]
        return pltpu.make_async_copy(others, others, sem.at[kind])

    def fold(carry, y):
        y = y.reshape(-1, LANES, 8, y.shape[-1])
        return carry[0] + jnp.sum(y, axis=0), carry[1] + jnp.sum(y * y, axis=0)

    def zeros(cols):
        zero = jnp.zeros((LANES, 8, cols), jnp.float32)
        return zero, zero

    order = sorted(range(1, n), key=lambda k: (1 - k % 2, -abs(2 * k - n)))

    def total(part):
        return jnp.sum(jnp.sum(part, axis=0), axis=0, keepdims=True)

    def send_stats(layer, kind, carry):
        stage = layer * stages + kind
        first = total(carry[0])
        both = jnp.concatenate([first, total(carry[1])], axis=0)
        cols = both.shape[-1]
        stat_out[stage, :, 0:cols] = both
        stat[stage, 0, :, 0:cols] = both
        for k in order:
            stat_copy(stage, kind, k).start()
        return first

    def affine(layer, kind, gain, shift):
        stage = layer * stages + kind
        all_stats(stage, kind, stat_recv).wait()
        cols = gain.shape[-1]
        both = jnp.sum(stat[stage], axis=0)[:, 0:cols]
        mean = both[0:1] * inv_count
        var = jnp.maximum(both[1:2] * inv_count - mean * mean, 0.0)
        scale = lax.rsqrt(var + EPS) * gain
        return scale, shift - mean * scale

    def halo_copy(layer, side):
        return pltpu.make_async_remote_copy(
            src_ref=halo_out.at[layer, side],
            dst_ref=halo_in.at[layer, 1 - side],
            send_sem=halo_send.at[side],
            recv_sem=halo_recv.at[1 - side],
            device_id={"slab": peer(n - 1 if side == 0 else 1)},
            device_id_type=MESH,
        )

    def halo_arrival(layer, side):
        return pltpu.make_async_remote_copy(
            src_ref=halo_out.at[layer, side],
            dst_ref=halo_in.at[layer, side],
            send_sem=halo_send.at[side],
            recv_sem=halo_recv.at[side],
            device_id={"slab": peer(n - 1 if side == 0 else 1)},
            device_id_type=MESH,
        )

    def has_neighbour(side):
        return me > 0 if side == 0 else me < n - 1

    edge = lax.broadcasted_iota(jnp.int32, (16, mid), 0)

    def store_taps(row, h):
        at = span(row)
        before = pltpu.roll(h, 1, 0)
        after = pltpu.roll(h, width - 1, 0)
        taps[at, mid : 2 * mid] = h.astype(jnp.bfloat16)
        before = jnp.concatenate([jnp.where(edge == 0, 0.0, before[0:16]), before[16:]], axis=0)
        taps[at, 0:mid] = before.astype(jnp.bfloat16)
        after = jnp.concatenate(
            [after[: width - 16], jnp.where(edge == 15, 0.0, after[width - 16 :])], axis=0
        )
        taps[at, 2 * mid : 3 * mid] = after.astype(jnp.bfloat16)

    def keep_sums(carry):
        sums[0] = carry[0]
        sums[1] = carry[1]

    for side in range(2):

        @pl.when(jnp.logical_not(has_neighbour(side)))
        def _():
            for layer in range(layers):
                halo_in[layer, side] = jnp.zeros((width, mid), jnp.bfloat16)

    weight_copy(0, 0).wait()
    carry = zeros(mid)
    for step, picks in enumerate(steps):
        x_arrival(step).wait()
        for r in picks:
            y = jnp.dot(
                jnp.concatenate([x[c, r] for c in range(chunks)], axis=1),
                wr[0],
                preferred_element_type=jnp.float32,
            )
            red[span(r), :] = y
            carry = fold(carry, y)
    keep_sums(carry)
    for copy in small:
        copy.wait()
    pl.semaphore_wait(barrier, n - 1)

    def layer_step(layer, _):
        first = layer * stages

        local_mean = send_stats(layer, 0, (sums[0], sums[1])) * inv_local
        for side in range(2):
            row = 0 if side == 0 else rows - 1
            halo_out[layer, side] = (red[span(row), :] - local_mean).astype(jnp.bfloat16)

            @pl.when(has_neighbour(side))
            def _():
                halo_copy(layer, side).start()

        weight_copy(1, layer).start()
        for c in range(chunks):
            expand_copy(layer, c).start()

        @pl.when(layer < layers - 1)
        def _():
            weight_copy(0, layer + 1).start()

        weight_copy(1, layer).wait()
        scale, shift = affine(layer, 0, gain_mid[layer, 0:1], shift_mid[layer, 0:1])

        def hidden(row):
            store_taps(row + 1, jnp.maximum(red[span(row), :] * scale + shift, 0.0))

        def conv(row, many):
            y = jnp.dot(
                jnp.concatenate([taps[span(row + down, many), :] for down in range(3)], axis=1),
                ws[layer].reshape(9 * mid, mid),
                preferred_element_type=jnp.float32,
            )
            red[span(row, many), :] = y
            return y

        def conv_edge(side, first, many):
            row = 0 if side == 0 else rows - 1
            return jnp.dot(
                jnp.concatenate([taps[span(row + first + i), :] for i in range(many)], axis=1),
                ws[layer, pl.ds(3 * first, 3 * many)].reshape(3 * many * mid, mid),
                preferred_element_type=jnp.float32,
            )

        carry = zeros(mid)
        done = 0
        conv_rows = divisor(rows - 2, CONV_ROWS)
        for row in range(1, rows - 1, conv_rows):
            while done < row + conv_rows + 1:
                hidden(done)
                done += 1
            for r in range(row, row + conv_rows):
                carry = fold(carry, conv(r, 1))
        for side in range(2):
            red[span(0 if side == 0 else rows - 1), :] = conv_edge(side, 1 - side, 2)

        for side in range(2):

            @pl.when(has_neighbour(side))
            def _():
                halo_copy(layer, side).wait_send()
                halo_arrival(layer, side).wait_recv()

        for side in range(2):
            row = 0 if side == 0 else rows + 1
            there = jnp.where(has_neighbour(side), 1.0, 0.0)
            y = halo_in[layer, side].astype(jnp.float32) * (scale * there)
            theirs = stat[first, 1 if side == 0 else n - 1, 0:1, 0:mid] * inv_local
            moved = theirs * scale + shift
            store_taps(row, jnp.maximum(y + moved * there, 0.0))

        for side in range(2):
            at = span(0 if side == 0 else rows - 1)
            y = conv_edge(side, 2 * side, 1) + red[at, :]
            red[at, :] = y
            carry = fold(carry, y)
        send_stats(layer, 1, carry)

        expand_arrival(layer).wait()
        scale, shift = affine(layer, 1, gain_mid[layer, 1:2], shift_mid[layer, 1:2])

        expand_rows = divisor(rows, EXPAND_ROWS)
        for g in range(groups):
            parts = [zeros(mid) for _ in range(group)]
            for row in range(0, rows, expand_rows):
                at = span(row, expand_rows)
                if g == 0:
                    block = jnp.maximum(red[at, :] * scale + shift, 0.0).astype(jnp.bfloat16)
                    inner[at, :] = block
                else:
                    block = inner[at, :]
                for i in range(group):
                    c = g * group + i
                    y = jnp.dot(
                        block, we[layer, c],
                        preferred_element_type=jnp.float32,
                    )
                    expanded[c, at, :] = y
                    parts[i] = fold(parts[i], y)
            send_stats(
                layer,
                2 + g,
                tuple(jnp.concatenate([p[j] for p in parts], axis=-1) for j in range(2)),
            )

        @pl.when(layer < layers - 1)
        def _():
            weight_copy(0, layer + 1).wait()

        carry = zeros(mid)
        for g in range(groups):
            cols = slice(g * wide, (g + 1) * wide)
            scale, shift = affine(
                layer, 2 + g, gain_out[pl.ds(layer, 1), cols], shift_out[pl.ds(layer, 1), cols]
            )

            @pl.when(layer == layers - 1)
            def _():
                if g == groups - 1:
                    last[0:1, :] = scale
                    last[1:2, :] = shift
                else:
                    for row in range(rows):
                        for c in range(g * group, (g + 1) * group):
                            part = slice((c - g * group) * mid, (c - g * group + 1) * mid)
                            y = expanded[c, span(row), :] * scale[:, part] + shift[:, part]
                            x[c, row] = jnp.maximum(y.astype(jnp.bfloat16) + x[c, row], 0.0)

            @pl.when(layer < layers - 1)
            def _():
                carry = zeros(mid)
                for row in range(rows):
                    at = span(row)
                    blocks = []
                    for i in range(group):
                        c = g * group + i
                        part = slice(i * mid, (i + 1) * mid)
                        y = expanded[c, at, :] * scale[:, part] + shift[:, part]
                        y = jnp.maximum(y.astype(jnp.bfloat16) + x[c, row], 0.0)
                        x[c, row] = y
                        blocks.append(y)
                    y = jnp.dot(
                        jnp.concatenate(blocks, axis=1),
                        wr[layer + 1, cols, :],
                        preferred_element_type=jnp.float32,
                    )
                    if g > 0:
                        y = y + red[at, :]
                    red[at, :] = y
                    if g == groups - 1:
                        carry = fold(carry, y)
                if g == groups - 1:
                    keep_sums(carry)

        for stage in range(stages):
            all_stats(first + stage, stage, stat_send).wait()
        return 0

    lax.fori_loop(0, layers, layer_step, 0)


def finish(expanded, x, last, out_hbm, buffer, out_sem):
    chunks, rows, width, mid = x.shape

    done = chunks - last.shape[1] // mid

    def out_copy(c):
        cols = pl.ds(c * mid, mid)
        return pltpu.make_async_copy(x.at[c], out_hbm.at[:, :, cols], out_sem.at[c])

    def row_copy(row):
        cols = pl.ds(done * mid, (chunks - done) * mid)
        return pltpu.make_async_copy(
            buffer.at[row], out_hbm.at[row, :, cols], out_sem.at[done + row]
        )

    for c in range(done):
        out_copy(c).start()
    for row in range(rows):
        at = pl.ds(row * width, width)
        for c in range(done, chunks):
            cols = slice((c - done) * mid, (c - done + 1) * mid)
            y = expanded[c, at, :] * last[0:1, cols] + last[1:2, cols]
            buffer[row, :, cols] = jnp.maximum(y.astype(jnp.bfloat16) + x[c, row], 0.0)
        row_copy(row).start()
    for c in range(done):
        out_copy(c).wait()
    for row in range(rows):
        row_copy(row).wait()


def solution(mesh):
    n = mesh.shape["slab"]

    def local(section_input, w_reduce, w_spatial, w_expand, gain_mid, shift_mid, gain_out, shift_out):
        rows, width, chans = section_input.shape
        layers, _, mid = w_reduce.shape
        chunks = chans // mid
        group = divisor(chunks, GROUP)
        count = rows * width
        stages = layers * (2 + chunks // group)
        wide = group * mid
        bf16, f32 = jnp.bfloat16, jnp.float32
        hbm = pl.BlockSpec(memory_space=pl.ANY)
        vmem = pl.BlockSpec(memory_space=pltpu.VMEM)
        held = pl.pallas_call(
            functools.partial(kernel, n),
            out_shape=[
                pltpu.VMEM((chunks, count, mid), f32),
                pltpu.VMEM((chunks, rows, width, mid), bf16),
                pltpu.VMEM((2, wide), f32),
            ],
            in_specs=[hbm] * 8,
            out_specs=[vmem] * 3,
            scratch_shapes=[
                pltpu.VMEM(gain_mid.shape, f32),
                pltpu.VMEM(shift_mid.shape, f32),
                pltpu.VMEM(gain_out.shape, f32),
                pltpu.VMEM(shift_out.shape, f32),
                pltpu.VMEM(w_reduce.shape, bf16),
                pltpu.VMEM(w_spatial.shape, bf16),
                pltpu.VMEM((layers, chunks, mid, mid), bf16),
                pltpu.VMEM((count, mid), f32),
                pltpu.VMEM(((rows + 2) * width, 3 * mid), bf16),
                pltpu.VMEM((count, mid), bf16),
                pltpu.VMEM((layers, 2, width, mid), bf16),
                pltpu.VMEM((layers, 2, width, mid), bf16),
                pltpu.VMEM((stages, 2, wide), f32),
                pltpu.VMEM((stages, n, 2, wide), f32),
                pltpu.VMEM((2, LANES, 8, mid), f32),
                pltpu.SemaphoreType.DMA((4,)),
                pltpu.SemaphoreType.DMA((max(1, rows // divisor(rows, REDUCE_ROWS) - 1),)),
                pltpu.SemaphoreType.DMA((3,)),
                pltpu.SemaphoreType.DMA((2,)),
                pltpu.SemaphoreType.DMA((2,)),
                pltpu.SemaphoreType.DMA((stages // layers,)),
                pltpu.SemaphoreType.DMA((stages // layers,)),
            ],
            compiler_params=pltpu.CompilerParams(
                collective_id=0, has_side_effects=True, vmem_limit_bytes=40 * 1024 * 1024
            ),
            name="blocks",
        )(
            *(
                pltpu.with_memory_space_constraint(a, pltpu.HBM)
                for a in (
                    section_input, w_reduce, w_spatial, w_expand,
                    gain_mid, shift_mid, gain_out, shift_out,
                )
            )
        )
        held = [pltpu.with_memory_space_constraint(a, pltpu.VMEM) for a in held]
        return pl.pallas_call(
            finish,
            out_shape=jax.ShapeDtypeStruct(section_input.shape, bf16),
            in_specs=[vmem] * 3,
            out_specs=hbm,
            scratch_shapes=[
                pltpu.VMEM((rows, width, wide), bf16),
                pltpu.SemaphoreType.DMA((chunks + rows,)),
            ],
            compiler_params=pltpu.CompilerParams(vmem_limit_bytes=16 * 1024 * 1024),
            name="finish",
        )(*held)

    placed = (P(("img", "slab"), None, None), P(), P(), P(), P(), P(), P(), P())
    return jax.shard_map(
        local, mesh=mesh, in_specs=placed, out_specs=P(("img", "slab"), None, None), check_vma=False
    )
```
